256 devices in a mesh: section: 8 (over y, core), expert: 32 (over z, x).
Axes of the slice: x: 4, y: 4, z: 8, core: 2. Of those that a mesh axis runs over, the one named last changes fastest.
Arguments:
- tokens: bfloat16 [2, 4096, 2048], P(None, 'expert'), may hold values from -6 to 6
- norm_gain: float32 [8, 2048], P('section'), may hold values from 0.1 to 1.9
- w_gate: bfloat16 [8, 32, 2048, 704], P('section', 'expert'), may hold values from -0.125 to 0.125
- w_up: bfloat16 [8, 32, 2048, 704], P('section', 'expert'), may hold values from -0.125 to 0.125
- w_down: bfloat16 [8, 32, 704, 2048], P('section', 'expert'), may hold values from -0.21875 to 0.21875
- expert_ids: int32 [8, 2, 4096, 6], P('section', None, 'expert'), may hold values from 0 to 31, all different within a row; in each aligned block of 128 rows (0 to 127, 128 to 255, ..., all dimensions but the last counted through in order) at most 25 rows name the same one
- route_weight: float32 [8, 2, 4096, 6], P('section', None, 'expert'), may hold values from 0.1 to 1
Outputs:
- stream: bfloat16 [8, 2, 4096, 2048], P('section', None, 'expert')
The draws below stay inside these ranges and needn't reach their ends.
Inputs may be any that keep to these rules, and one draw needn't show every extreme that they name: `expert_ids`: A token names 6 different experts. In each aligned block of 128 tokens (the tokens of one device in one layer and micro-batch) no expert is named by more than 25 tokens, a bound that some block reaches.
All inputs are finite; a program needn't handle non-finite values.
Results may differ from the reference program's by a relative error of at most 0.025.
Values may be sent and summed in bfloat16 or wider, within the bound.
A program may use at most 128 MiB of HBM per device.

```python
import math
import jax
import jax.numpy as jnp
import numpy as np
from jax import lax

D = 2048
HID = 704
TOP = 6
MB = 2
TOK_DEV = 128
EXPERTS = 32
LAYERS = 8
TOKENS = 4096
CAP = 25
N_EXPERT = 32


def block_scale(own_key, extent, pieces, least, high):
    loudness, own = 1.0, jax.random.fold_in(own_key, 6)
    for position, shards_of in pieces:
        draws = jnp.exp(jax.random.uniform(jax.random.fold_in(own, position), (shards_of,), jnp.float32, least / len(pieces), high / len(pieces)))
        loudness = loudness * jnp.repeat(draws, extent[position] // shards_of).reshape([-1 if axis == position else 1 for axis in range(len(extent))])
    return loudness


def deal_out(key, own, number, rows, amount, top, most, skew):
    order = jax.random.permutation(key, amount)
    heavy_load, common = load_shares(amount, rows * top, most, skew, True), load_shares(amount, rows * top, most, skew, False)
    places = jnp.arange(amount)

    def named(tallies, offset_by):
        used = int((tallies > 0).sum())
        fixed = max(1, used // 4)
        moved = fixed + (places - fixed + offset_by * (used - fixed)) % max(1, amount - fixed)
        return jnp.zeros((amount,), jnp.int32).at[order[jnp.where(places < fixed, places, moved)]].set(jnp.asarray(tallies, jnp.int32))

    tallies = jnp.where(number % 4 == 0, named(heavy_load, number // 4), named(common, number - number // 4 - 1))
    mixed = jax.random.permutation(jax.random.fold_in(own, 3), amount)
    donor, sink = mixed[0:amount // 2 * 2:2], mixed[1:amount // 2 * 2:2]
    room = jnp.minimum(tallies[donor] - 1, most - tallies[sink]) // 2
    room = jnp.where((donor == order[0]) | (sink == order[0]) | (tallies[sink] == 0), 0, jnp.maximum(room, 0))
    moved = jax.random.randint(jax.random.fold_in(own, 4), (amount // 2,), 0, 1 << 20) % (room + 1)
    tallies = tallies.at[donor].add(-moved).at[sink].add(moved)
    members = jnp.searchsorted(jnp.cumsum(tallies), jnp.arange(rows * top), side="right").astype(jnp.int32)
    listing = members.reshape(top, rows).T
    listing = listing[jax.random.permutation(jax.random.fold_in(own, 1), rows)]
    offset_by = jax.random.randint(jax.random.fold_in(own, 2), (rows, 1), 0, top)
    return jnp.take_along_axis(listing, (jnp.arange(top)[None, :] + offset_by) % top, axis=1)


def load_shares(amount, total, reach, slope, full):
    weights = [(1 << 20) // math.isqrt(grade ** slope) + 1 for grade in range(1, amount + 1)]
    largest = reach if full else min(reach, max(-(-total // amount), total * weights[0] // sum(weights)))
    least = 1 if total - largest >= amount - 1 else 0
    counts, rest = [largest] + [least] * (amount - 1), total - largest - least * (amount - 1)
    while rest > 0:
        free = [i for i in range(1, amount) if counts[i] < largest] or [i for i in range(1, amount) if counts[i] < reach]
        whole, budget = sum([weights[i] for i in free]), rest
        for i in free:
            more = min(reach - counts[i], max(1, budget * weights[i] // whole), rest)
            counts[i] = counts[i] + more
            rest = rest - more
    return np.array(counts)


def scatter_about(stream_key, shape, spread, bound, cuts=(), held_as=jnp.bfloat16):
    result = jax.random.normal(stream_key, shape, jnp.float32) * spread
    if len(cuts) > 0:
        result = block_scale(stream_key, shape, cuts, -0.22, 0.18) * result
    return jnp.clip(result, min=-bound, max=bound).astype(held_as)


def setup_inputs(seed: int = 0) -> dict:
    seeds = jax.random.split(jax.random.key(seed), 8)
    tokens = scatter_about(seeds[0], (MB, TOKENS, D), 1.0, 6.0, ((1, 32),))
    norm_gain = jnp.clip(1.0 + 0.18 * jax.random.normal(seeds[1], (LAYERS, D), jnp.float32), 0.1, 1.9)
    w_gate = scatter_about(seeds[2], (LAYERS, EXPERTS, D, HID), D ** -0.5, 0.125, ((0, 8), (1, 32)))
    w_up = scatter_about(seeds[3], (LAYERS, EXPERTS, D, HID), D ** -0.5, 0.125, ((0, 8), (1, 32)))
    w_down = scatter_about(seeds[4], (LAYERS, EXPERTS, HID, D), HID ** -0.5, 0.21875, ((0, 8), (1, 32)))
    expert_ids_keys = jax.random.split(jax.random.fold_in(seeds[5], 1), LAYERS * MB * TOKENS // TOK_DEV)
    expert_ids_turns = jax.random.permutation(jax.random.fold_in(seeds[5], 3), LAYERS * MB * TOKENS // TOK_DEV)
    expert_ids = jax.vmap(lambda own, number: deal_out(jax.random.fold_in(seeds[5], 2), own, number, TOK_DEV, EXPERTS, TOP, CAP, 0))(expert_ids_keys, expert_ids_turns).reshape((LAYERS, MB, TOKENS, TOP))
    route_weight = jnp.clip(jnp.exp(math.log(1.0) - 2.3025851 * jax.random.uniform(seeds[6], (LAYERS, MB, TOKENS, TOP), jnp.float32) ** block_scale(seeds[6], (LAYERS, MB, TOKENS, TOP), ((0, 8), (2, 32)), -0.2, 0.2)), 0.1, 1.0)
    return {"tokens": tokens, "norm_gain": norm_gain, "w_gate": w_gate, "w_up": w_up, "w_down": w_down, "expert_ids": expert_ids, "route_weight": route_weight}


epsilon = 1e-06

def expert_mlp(operands):
    inputs, gate_matrix, up_matrix, down_matrix = operands
    gate_proj = jnp.dot(inputs, gate_matrix, preferred_element_type=jnp.float32)
    upward = jnp.dot(inputs, up_matrix, preferred_element_type=jnp.float32)
    hidden = (jax.nn.silu(gate_proj) * upward).astype(jnp.bfloat16)
    return jnp.dot(hidden, down_matrix, preferred_element_type=jnp.float32).astype(jnp.bfloat16)

def layer_apply(residual, norm_scale, gate_all, up_all, down_all, route_ids, weights):
    values = residual.astype(jnp.float32)
    inverse_rms = lax.rsqrt(lax.optimization_barrier(jnp.mean(values * values, axis=-1, keepdims=True)) + epsilon)
    normed = (values * inverse_rms * norm_scale).astype(jnp.bfloat16)
    grouped = route_ids.reshape(N_EXPERT, TOK_DEV * TOP)
    onehot = (grouped[:, :, None] == jnp.arange(EXPERTS, dtype=jnp.int32)[None, None, :]).astype(jnp.int32)
    slot_index = lax.optimization_barrier(jnp.sum((jnp.cumsum(onehot, axis=1) - 1) * onehot, axis=-1))
    target = (jnp.arange(N_EXPERT, dtype=jnp.int32)[:, None] * CAP + slot_index).reshape(-1).astype(jnp.int32)
    chosen = route_ids.reshape(-1).astype(jnp.int32)
    owners = (jnp.arange(TOKENS * TOP, dtype=jnp.int32) // TOP).astype(jnp.int32)
    buffers = jnp.zeros((EXPERTS, N_EXPERT * CAP, D), jnp.bfloat16).at[chosen, target].set(normed[owners])
    results = lax.map(expert_mlp, (buffers, gate_all, up_all, down_all))
    picked = results[chosen, target].reshape(TOKENS, TOP, D).astype(jnp.float32)
    combined = values + lax.optimization_barrier(jnp.sum(weights[:, :, None] * picked, axis=1))
    return combined.astype(jnp.bfloat16)

def reference(tokens, norm_gain, w_gate, w_up, w_down, expert_ids, route_weight):
    states = [tokens[index] for index in range(MB)]
    layer_rows = []
    for layer in range(LAYERS):
        micro_rows = []
        for index in range(MB):
            states[index] = layer_apply(states[index], norm_gain[layer], w_gate[layer], w_up[layer], w_down[layer], expert_ids[layer, index], route_weight[layer, index])
            micro_rows.append(states[index])
        layer_rows.append(jnp.stack(micro_rows))
    return jnp.stack(layer_rows)
```

```python
import functools

import jax
import jax.numpy as jnp
from jax import lax
from jax.experimental import pallas as pl
from jax.experimental.pallas import tpu as pltpu
from jax.sharding import PartitionSpec as P

EPSILON = 1e-06
X_SIZE = 4
SLOT = 32
LANES = 128
COLS = 512
MESH = pl.DeviceIdType.MESH


def relay_kernel(
    sections,
    ring,
    tokens,
    gain,
    w_gate,
    w_up,
    w_down,
    ids,
    route,
    out,
    ag,
    xs,
    xr,
    ret,
    abuf,
    bbuf,
    hop,
    comb,
    z_send,
    z_recv,
    x_send,
    x_recv,
    r_send,
    r_recv,
    a_send,
    a_recv,
    b_send,
    b_recv,
    h_send,
    h_recv,
):
    micro, rows, width = tokens.shape
    top = ids.shape[-1]
    experts = ring * X_SIZE
    far_a = ring // 2
    far_b = ring // 2 - 1
    tiles = width // COLS
    sec = lax.axis_index("section")
    pos = lax.axis_index("expert")
    z = pos // X_SIZE
    x = pos % X_SIZE
    right = ((z + 1) % ring) * X_SIZE + x
    left = ((z + ring - 1) % ring) * X_SIZE + x

    def x_peer(offset):
        return z * X_SIZE + (x + offset) % X_SIZE

    barrier = pltpu.get_barrier_semaphore()
    for peer in [right, left] + [x_peer(o) for o in range(1, X_SIZE)]:
        pl.semaphore_signal(barrier, inc=1, device_id=(sec, peer), device_id_type=MESH)
    for other in [(sec + 1) % sections, (sec + sections - 1) % sections]:
        pl.semaphore_signal(barrier, inc=1, device_id=(other, pos), device_id_type=MESH)
    pl.semaphore_wait(barrier, X_SIZE + 3)

    def remote(src, dst, send, recv, where):
        return pltpu.make_async_remote_copy(
            src_ref=src,
            dst_ref=dst,
            send_sem=send,
            recv_sem=recv,
            device_id=where,
            device_id_type=MESH,
        )

    def z_copy(m, frm, to, peer):
        return remote(
            ag.at[m, frm], ag.at[m, to], z_send.at[m, to], z_recv.at[m, to], (sec, peer)
        )

    def lump(j, d):
        return pl.ds(pl.multiple_of(j * LANES + d * SLOT, SLOT), SLOT)

    def x_copy(m, j, o):
        return remote(
            xs.at[m, lump(j, (x + o) % X_SIZE)],
            xr.at[m, lump(j, x)],
            x_send.at[m, j, o - 1],
            x_recv.at[m, j, o - 1],
            (sec, x_peer(o)),
        )

    def r_copy(m, j, o):
        return remote(
            xr.at[m, lump(j, (x + o) % X_SIZE)],
            ret.at[m, lump(j, x)],
            r_send.at[m, j, o - 1],
            r_recv.at[m, j, o - 1],
            (sec, x_peer(o)),
        )

    def a_copy(m, r):
        return remote(
            abuf.at[m, r], abuf.at[m, r + 1], a_send.at[m, r], a_recv.at[m, r], (sec, left)
        )

    def b_copy(m, r):
        return remote(
            bbuf.at[m, r], bbuf.at[m, r + 1], b_send.at[m, r], b_recv.at[m, r], (sec, right)
        )

    def h_copy(m, c):
        cols = pl.ds(c * COLS, COLS)
        return remote(
            out.at[m, :, cols],
            hop.at[m, :, cols],
            h_send.at[m, c],
            h_recv.at[m, c],
            ((sec + 1) % sections, pos),
        )

    lane = lax.broadcasted_iota(jnp.int32, (LANES, LANES), 1)
    line = lax.broadcasted_iota(jnp.int32, (LANES, LANES), 0)
    mine = z * X_SIZE + lane // SLOT
    spread_slot = (line == mine).astype(jnp.bfloat16)
    spread_weight = (line == mine + experts).astype(jnp.bfloat16)
    slot_of_lane = (lane % SLOT).astype(jnp.float32)
    earlier = (lane < line).astype(jnp.bfloat16)

    def dot(a, b):
        return jnp.dot(a, b, preferred_element_type=jnp.float32)

    def col_loop(body):
        @pl.loop(0, tiles)
        def _(c):
            body(pl.ds(pl.multiple_of(c * COLS, COLS), COLS))

    def pick_rows(m, j):
        meta = ag[m, j, :, width:]
        hit = dot(meta, spread_slot) == slot_of_lane
        comb[j] = jnp.where(hit, dot(meta, spread_weight), 0.0).astype(jnp.bfloat16)
        pick = jnp.transpose(hit.astype(jnp.float32)).astype(jnp.bfloat16)
        block = pl.ds(pl.multiple_of(j * LANES, LANES), LANES)

        def tile(cols):
            xs[m, block, cols] = dot(pick, ag[m, j, :, cols]).astype(jnp.bfloat16)

        col_loop(tile)
        for o in range(1, X_SIZE):
            x_copy(m, j, o).start()
        xr[m, lump(j, x), :] = xs[m, lump(j, x), :]

    def expert(m, g):
        for j in (2 * g, 2 * g + 1):
            for o in range(1, X_SIZE):
                x_copy(m, j, o).wait_recv()
        group = pl.ds(pl.multiple_of(g * 2 * LANES, 2 * LANES), 2 * LANES)
        gate = dot(xr[m, group, :], w_gate[...])
        up = dot(xr[m, group, :], w_up[...])
        act = (gate / (1.0 + jnp.exp(-gate)) * up).astype(jnp.bfloat16)

        def tile(cols):
            xr[m, group, cols] = dot(act, w_down[:, cols]).astype(jnp.bfloat16)

        col_loop(tile)
        for j in (2 * g, 2 * g + 1):
            for o in range(1, X_SIZE):
                r_copy(m, j, o).start()
            ret[m, lump(j, x), :] = xr[m, lump(j, x), :]

    def returned(m, j):
        for o in range(1, X_SIZE):
            r_copy(m, j, o).wait_recv()

    def combined(m, j, cols):
        block = pl.ds(pl.multiple_of(j * LANES, LANES), LANES)
        return dot(comb[j], ret[m, block, cols])

    @pl.when(sec == 0)
    def _():
        @pl.loop(0, micro * rows // 16)
        def _(i):
            m = i // (rows // 16)
            r = pl.ds(pl.multiple_of((i % (rows // 16)) * 16, 16), 16)
            hop[m, r, :] = tokens[m, r, :]

    @pl.loop(0, micro)
    def _(m):
        @pl.when(sec > 0)
        def _():
            for c in range(tiles):
                h_copy(m, c).wait_recv()

        @pl.loop(0, rows // 16)
        def _(i):
            r = pl.ds(pl.multiple_of(i * 16, 16), 16)
            value = hop[m, r, :].astype(jnp.float32)
            inverse = lax.rsqrt(jnp.mean(value * value, axis=-1, keepdims=True) + EPSILON)
            ag[m, 0, r, :width] = (value * inverse * gain[...]).astype(jnp.bfloat16)

        member = jnp.zeros((rows, LANES), jnp.float32)
        weight = jnp.zeros((rows, LANES), jnp.float32)
        for k in range(top):
            choice = ids[m, :, k : k + 1]
            member = member + (choice == lane).astype(jnp.float32)
            weight = weight + jnp.where(choice + experts == lane, route[m, :, k : k + 1], 0.0)
        before = dot(earlier, member.astype(jnp.bfloat16))
        slot = jnp.where(member > 0.0, before, -1.0)
        ag[m, 0, :, width:] = jnp.where(lane < experts, slot, weight).astype(jnp.bfloat16)

        z_copy(m, 0, 1, right).start()
        z_copy(m, 0, 2, left).start()
        pick_rows(m, 0)

        @pl.loop(1, far_a + 2)
        def _(k):
            @pl.when(k <= far_a)
            def _():
                near = 2 * k - 1
                z_copy(m, near, near, right).wait_recv()

                @pl.when(k < far_a)
                def _():
                    z_copy(m, near, near + 2, right).start()

                @pl.when(k <= far_b)
                def _():
                    z_copy(m, near + 1, near + 1, left).wait_recv()

                    @pl.when(k < far_b)
                    def _():
                        z_copy(m, near + 1, near + 3, left).start()

                pick_rows(m, near)

                @pl.when(k <= far_b)
                def _():
                    pick_rows(m, near + 1)

            @pl.when(k >= 2)
            def _():
                expert(m, k - 2)

        @pl.loop(0, far_a)
        def _(r):
            ja = 2 * (far_a - r) - 1
            returned(m, ja)

            @pl.when(r == 0)
            def _():
                def tile(cols):
                    abuf[m, r, :, cols] = combined(m, ja, cols).astype(jnp.bfloat16)

                col_loop(tile)

            @pl.when(r > 0)
            def _():
                a_copy(m, r - 1).wait_recv()

                def tile(cols):
                    abuf[m, r, :, cols] = (
                        abuf[m, r, :, cols].astype(jnp.float32) + combined(m, ja, cols)
                    ).astype(jnp.bfloat16)

                col_loop(tile)

            a_copy(m, r).start()

            @pl.when(r < far_b)
            def _():
                jb = 2 * (far_b - r)
                returned(m, jb)

                @pl.when(r == 0)
                def _():
                    def tile(cols):
                        bbuf[m, r, :, cols] = combined(m, jb, cols).astype(jnp.bfloat16)

                    col_loop(tile)

                @pl.when(r > 0)
                def _():
                    b_copy(m, r - 1).wait_recv()

                    def tile(cols):
                        bbuf[m, r, :, cols] = (
                            bbuf[m, r, :, cols].astype(jnp.float32) + combined(m, jb, cols)
                        ).astype(jnp.bfloat16)

                    col_loop(tile)

                b_copy(m, r).start()

        returned(m, 0)
        b_copy(m, far_b - 1).wait_recv()
        a_copy(m, far_a - 1).wait_recv()
        for c in range(tiles):
            cols = pl.ds(c * COLS, COLS)
            total = (
                combined(m, 0, cols)
                + abuf[m, far_a, :, cols].astype(jnp.float32)
                + bbuf[m, far_b, :, cols].astype(jnp.float32)
            )
            out[m, :, cols] = (hop[m, :, cols].astype(jnp.float32) + total).astype(jnp.bfloat16)

            @pl.when(sec < sections - 1)
            def _():
                h_copy(m, c).start()

    @pl.loop(0, micro)
    def _(m):
        for j in range(1, ring):
            z_copy(m, j, j, right).wait_send()
        for j in range(ring):
            for o in range(1, X_SIZE):
                x_copy(m, j, o).wait_send()
                r_copy(m, j, o).wait_send()
        for r in range(far_a):
            a_copy(m, r).wait_send()
        for r in range(far_b):
            b_copy(m, r).wait_send()

        @pl.when(sec < sections - 1)
        def _():
            for c in range(tiles):
                h_copy(m, c).wait_send()


def per_device(tokens, norm_gain, w_gate, w_up, w_down, expert_ids, route_weight):
    sections = lax.axis_size("section")
    ring = lax.axis_size("expert") // X_SIZE
    micro, rows, width = tokens.shape
    block = (micro, ring * LANES, width)
    dma = pltpu.SemaphoreType.DMA
    result = pl.pallas_call(
        functools.partial(relay_kernel, sections, ring),
        out_shape=jax.ShapeDtypeStruct((micro, rows, width), jnp.bfloat16),
        in_specs=[pl.BlockSpec(memory_space=pltpu.VMEM)] * 7,
        out_specs=pl.BlockSpec(memory_space=pltpu.VMEM),
        scratch_shapes=[
            pltpu.VMEM((micro, ring, rows, width + LANES), jnp.bfloat16),
            pltpu.VMEM(block, jnp.bfloat16),
            pltpu.VMEM(block, jnp.bfloat16),
            pltpu.VMEM(block, jnp.bfloat16),
            pltpu.VMEM((micro, ring // 2 + 1, rows, width), jnp.bfloat16),
            pltpu.VMEM((micro, ring // 2, rows, width), jnp.bfloat16),
            pltpu.VMEM((micro, rows, width), jnp.bfloat16),
            pltpu.VMEM((ring, rows, LANES), jnp.bfloat16),
            dma((micro, ring)),
            dma((micro, ring)),
            dma((micro, ring, X_SIZE - 1)),
            dma((micro, ring, X_SIZE - 1)),
            dma((micro, ring, X_SIZE - 1)),
            dma((micro, ring, X_SIZE - 1)),
            dma((micro, ring // 2)),
            dma((micro, ring // 2)),
            dma((micro, ring // 2)),
            dma((micro, ring // 2)),
            dma((micro, width // COLS)),
            dma((micro, width // COLS)),
        ],
        compiler_params=pltpu.CompilerParams(
            collective_id=0, has_side_effects=True, vmem_limit_bytes=67_000_000
        ),
        name="relay",
    )(
        tokens,
        norm_gain,
        w_gate[0, 0],
        w_up[0, 0],
        w_down[0, 0],
        expert_ids[0],
        route_weight[0],
    )
    return result[None]


def solution(mesh):
    return jax.shard_map(
        per_device,
        mesh=mesh,
        in_specs=(
            P(None, "expert", None),
            P("section", None),
            P("section", "expert", None, None),
            P("section", "expert", None, None),
            P("section", "expert", None, None),
            P("section", None, "expert", None),
            P("section", None, "expert", None),
        ),
        out_specs=P("section", None, "expert", None),
        check_vma=False,
    )
```

```python
import functools

import jax
import jax.numpy as jnp
from jax import lax
from jax.experimental import pallas as pl
from jax.experimental.pallas import tpu as pltpu
from jax.sharding import PartitionSpec as P

EPSILON = 1e-06
X_SIZE = 4
Y_SIZE = 4
CORES = 2
RING = 8
SLOT = 32
LANES = 128
COLS = 512
PIECES = 4
MESH = pl.DeviceIdType.MESH
LAG = 2
START_GROUPS = PIECES + LAG
FAR_A = RING // 2
FAR_B = RING // 2 - 1


def relay_kernel(
    tokens,
    gains,
    w_gate,
    w_up,
    w_down,
    ids,
    route,
    out,
    f_gate,
    f_up,
    f_down,
    v_gate,
    v_up,
    v_down,
    local_meta,
    meta,
    ag,
    xs,
    xr,
    ret,
    comb,
    part,
    abuf,
    bbuf,
    obuf,
    y_send,
    y_recv,
    d_send,
    d_recv,
    m_send,
    m_recv,
    t_send,
    t_recv,
    z_send,
    z_recv,
    x_send,
    x_recv,
    r_send,
    r_recv,
    a_send,
    a_recv,
    b_send,
    b_recv,
    o_send,
    o_recv,
    v_sem,
):
    micro, rows, width = tokens.shape
    own = rows // Y_SIZE
    top = ids.shape[-1]
    experts = RING * X_SIZE
    layers = Y_SIZE * CORES
    lumps = 2 * SLOT
    every = RING * own
    tiles = width // COLS
    sec = lax.axis_index("section")
    pos = lax.axis_index("expert")
    y = sec // CORES
    c = sec % CORES
    z = pos // X_SIZE
    x = pos % X_SIZE
    half = z // Y_SIZE
    quarter = z % Y_SIZE

    def at(zz):
        return ((zz + 2 * RING) % RING) * X_SIZE + x

    right = at(z + 1)
    left = at(z - 1)
    sibling = y * CORES + 1 - c
    y_peer = [((y + 1) % Y_SIZE) * CORES + c, ((y + Y_SIZE - 1) % Y_SIZE) * CORES + c]

    def remote(src, dst, send, recv, where):
        return pltpu.make_async_remote_copy(
            src_ref=src,
            dst_ref=dst,
            send_sem=send,
            recv_sem=recv,
            device_id=where,
            device_id_type=MESH,
        )

    def dot(a, b):
        return jnp.dot(a, b, preferred_element_type=jnp.float32)

    def dot_t(a, b):
        return lax.dot_general(
            a, b, (((1,), (1,)), ((), ())), preferred_element_type=jnp.float32
        )

    def col_loop(body):
        @pl.loop(0, tiles)
        def _(i):
            body(pl.ds(pl.multiple_of(i * COLS, COLS), COLS))

    given = (w_gate, w_up, w_down)
    full = (f_gate, f_up, f_down)
    step = (
        w_gate.shape[0] // (2 * PIECES),
        w_up.shape[0] // (2 * PIECES),
        w_down.shape[0] // (2 * PIECES),
    )

    def part_rows(t, i, d):
        return pl.ds(pl.multiple_of((d * PIECES + i) * step[t], step[t]), step[t])

    def y_copy(src, q, i, d, t):
        r = part_rows(t, i, d)
        return remote(
            src.at[r],
            full[t].at[2 * q + c, r],
            y_send.at[q, i, d, t],
            y_recv.at[q, i, d, t],
            (y_peer[d], pos),
        )

    def d_copy(src, q, i, d, t):
        r = part_rows(t, i, d)
        return remote(
            src.at[r],
            full[t].at[2 * q + c, r],
            d_send.at[q, i, d, t],
            d_recv.at[q, i, d, t],
            (sibling, pos),
        )

    def away_from(q, d):
        return (y - q + Y_SIZE) % Y_SIZE if d == 0 else (q - y + Y_SIZE) % Y_SIZE

    def stream(group, s):
        for k in range(Y_SIZE):
            t = (s - LAG * k) % 3
            g = group + (s - LAG * k) // 3
            valid = jnp.logical_and(g >= 0, g < Y_SIZE * PIECES)
            g = jnp.maximum(g, 0)
            q = g // PIECES
            i = g % PIECES
            for d in range(2):

                @pl.when(jnp.logical_and(valid, away_from(q, d) == k))
                def _():
                    held = given[t] if k == 0 else full[t].at[2 * q + c]
                    if k > 0:
                        y_copy(held, q, i, d, t).wait_recv()
                    if k < Y_SIZE - 1:
                        y_copy(held, q, i, d, t).start()
                    d_copy(held, q, i, d, t).start()

    def stream_done(q, i):
        for d in range(2):
            away = away_from(q, d)
            for t in range(3):
                held = full[t].at[2 * q + c]

                @pl.when(away < Y_SIZE - 1)
                def _():
                    y_copy(held, q, i, d, t).wait_send()

                d_copy(held, q, i, d, t).wait_send()

    def v_copy(src, dst, t):
        return pltpu.make_async_copy(src, dst, v_sem.at[t])

    held_v = (v_gate, v_up, v_down)

    def load_weights(layer):
        q = layer // 2

        @pl.when(layer % 2 != c)
        def _():
            for i in range(PIECES):
                for d in range(2):
                    for t in range(3):
                        r = part_rows(t, i, d)
                        remote(
                            full[t].at[layer, r],
                            full[t].at[layer, r],
                            d_send.at[q, i, d, t],
                            d_recv.at[q, i, d, t],
                            (sibling, pos),
                        ).wait_recv()

        @pl.when(layer == sec)
        def _():
            for t in range(3):
                v_copy(given[t], held_v[t], t).start()

        @pl.when(layer != sec)
        def _():
            for t in range(3):
                v_copy(full[t].at[layer], held_v[t], t).start()

    def weights_ready(layer):
        for t in range(3):
            v_copy(full[t].at[layer], held_v[t], t).wait()

    lane = lax.broadcasted_iota(jnp.int32, (rows, LANES), 1)
    line = lax.broadcasted_iota(jnp.int32, (rows, LANES), 0)
    earlier = (lane < line).astype(jnp.bfloat16)

    def m_copy(m, zz):
        return remote(
            local_meta.at[m],
            meta.at[sec, half],
            m_send.at[m, zz],
            m_recv.at[sec, half],
            (quarter * CORES + m, at(zz)),
        )

    def m_is_self(m, zz):
        return jnp.logical_and(quarter * CORES + m == sec, zz == z)

    for m in range(micro):
        member = jnp.zeros((rows, LANES), jnp.float32)
        weight = jnp.zeros((rows, LANES), jnp.float32)
        for k in range(top):
            choice = ids[m, :, k : k + 1]
            member = member + (choice == lane).astype(jnp.float32)
            weight = weight + jnp.where(choice + experts == lane, route[m, :, k : k + 1], 0.0)
        before = dot(earlier, member.astype(jnp.bfloat16))
        slot = jnp.where(member > 0.0, before, -1.0)
        local_meta[m] = jnp.where(lane < experts, slot, weight).astype(jnp.bfloat16)

    def t_copy(i):
        return remote(
            tokens.at[c, pl.ds(i * own, own)],
            obuf.at[1],
            t_send.at[i],
            t_recv,
            (sec, at(half * Y_SIZE + i)),
        )

    for i in range(Y_SIZE):

        @pl.when(jnp.logical_and(quarter == y, quarter != i))
        def _():
            t_copy(i).start()

        @pl.when(jnp.logical_and(quarter == y, quarter == i))
        def _():
            obuf[1] = tokens[c, pl.ds(i * own, own), :]

    for m in range(micro):
        for zz in range(RING):

            @pl.when(jnp.logical_not(m_is_self(m, zz)))
            def _():
                m_copy(m, zz).start()

            @pl.when(m_is_self(m, zz))
            def _():
                meta[sec, half] = local_meta[m]

    @pl.loop(0, START_GROUPS)
    def _(g):
        for s in range(3):
            stream(g, s)

    @pl.when(quarter != y)
    def _():
        t_copy(0).wait_recv()

    wide = 4 * lumps
    w_lane = lax.broadcasted_iota(jnp.int32, (LANES, wide), 1)
    w_line = lax.broadcasted_iota(jnp.int32, (LANES, wide), 0)
    target = z * X_SIZE + w_lane // lumps
    spread_slot = (w_line == target).astype(jnp.bfloat16)
    spread_weight = (w_line == target + experts).astype(jnp.bfloat16)
    g_lane = lax.broadcasted_iota(jnp.int32, (rows, wide), 1)
    slot_of_lane = (g_lane % SLOT).astype(jnp.float32)
    block_of_lane = (g_lane // SLOT) % 2

    def rows_of(zz):
        return pl.ds(pl.multiple_of(((zz + 2 * RING) % RING) * own, own), own)

    def z_copy(p, k, d, src):
        return remote(
            ag.at[p, rows_of(src)],
            ag.at[p, rows_of(src)],
            z_send.at[p, d, k],
            z_recv.at[p, d, k],
            (sec, (right, left)[d]),
        )

    def lump(d):
        return pl.ds(pl.multiple_of(d * lumps, lumps), lumps)

    def x_copy(p, o):
        return remote(
            xs.at[p, lump((x + o) % X_SIZE)],
            xr.at[p, lump(x)],
            x_send.at[p, o - 1],
            x_recv.at[p, o - 1],
            (sec, z * X_SIZE + (x + o) % X_SIZE),
        )

    def r_copy(p, o):
        return remote(
            xr.at[p, lump((x + o) % X_SIZE)],
            ret.at[p, lump(x)],
            r_send.at[p, o - 1],
            r_recv.at[p, o - 1],
            (sec, z * X_SIZE + (x + o) % X_SIZE),
        )

    def a_copy(p, r):
        return remote(
            abuf.at[p, r], abuf.at[p, r + 1], a_send.at[p, r], a_recv.at[p, r], (sec, left)
        )

    def b_copy(p, r):
        return remote(
            bbuf.at[p, r], bbuf.at[p, r + 1], b_send.at[p, r], b_recv.at[p, r], (sec, right)
        )

    home = half * Y_SIZE + y

    def o_copy(p, layer):
        return remote(
            obuf.at[p],
            out.at[c, pl.ds(pl.multiple_of(quarter * own, own), own)],
            o_send.at[p],
            o_recv.at[c, quarter],
            (layer, at(home)),
        )

    def o_is_self(layer):
        return jnp.logical_and(layer == sec, home == z)

    def sends_done(p, layer):
        for k in range(1, FAR_A + 1):
            z_copy(p, k, 0, z).wait_send()
        for k in range(1, FAR_B + 1):
            z_copy(p, k, 1, z).wait_send()
        for o in range(1, X_SIZE):
            x_copy(p, o).wait_send()
            r_copy(p, o).wait_send()
        for r in range(FAR_A):
            a_copy(p, r).wait_send()
        for r in range(FAR_B):
            b_copy(p, r).wait_send()

        @pl.when(jnp.logical_not(o_is_self(layer)))
        def _():
            o_copy(p, layer).wait_send()

    def streams(layer, lo, hi):
        @pl.when(layer < layers - 2)
        def _():
            for s in range(lo, hi):
                stream(START_GROUPS + 2 * layer + s // 3, s % 3)

    @pl.loop(0, layers)
    def _(layer):
        p = layer % 2

        value = obuf[1 - p].astype(jnp.float32)
        inverse = lax.rsqrt(jnp.mean(value * value, axis=-1, keepdims=True) + EPSILON)
        gain = gains[pl.ds(layer, 1), :]
        ag[p, rows_of(z), :] = (value * inverse * gain).astype(jnp.bfloat16)
        z_copy(p, 1, 0, z).start()
        z_copy(p, 1, 1, z).start()
        load_weights(layer)
        streams(layer, 0, 2)
        for h in range(2):

            @pl.when(jnp.logical_not(jnp.logical_and(layer == sec, home - half * Y_SIZE + h * Y_SIZE == z)))
            def _():
                remote(
                    meta.at[layer, h],
                    meta.at[layer, h],
                    m_send.at[0, 0],
                    m_recv.at[layer, h],
                    (sec, right),
                ).wait_recv()

        for k in range(1, FAR_A + 1):
            z_copy(p, k, 0, z - k).wait_recv()
            if k < FAR_A:
                z_copy(p, k + 1, 0, z - k).start()
            if k <= FAR_B:
                z_copy(p, k, 1, z + k).wait_recv()
                if k < FAR_B:
                    z_copy(p, k + 1, 1, z + k).start()

        @pl.when(layer >= 1)
        def _():
            sends_done(1 - p, layer - 1)

        for h in range(2):
            table = meta[layer, h]
            hit = jnp.logical_and(dot(table, spread_slot) == slot_of_lane, block_of_lane == h)
            scaled = jnp.where(hit, dot(table, spread_weight), 0.0)
            comb[0, pl.ds(h * rows, rows), :] = hit.astype(jnp.float32).astype(jnp.bfloat16)
            comb[1, pl.ds(h * rows, rows), :] = scaled.astype(jnp.bfloat16)
        pick = jnp.transpose(comb[0].astype(jnp.float32)).astype(jnp.bfloat16)

        def pick_tile(cols):
            xs[p, :, cols] = dot(pick, ag[p, :, cols]).astype(jnp.bfloat16)

        col_loop(pick_tile)
        for o in range(1, X_SIZE):
            x_copy(p, o).start()
        xr[p, lump(x), :] = xs[p, lump(x), :]
        streams(layer, 2, 4)
        weights_ready(layer)
        for o in range(1, X_SIZE):
            x_copy(p, o).wait_recv()

        gate = dot_t(xr[p], v_gate[...])
        up = dot_t(xr[p], v_up[...])
        act = (gate / (1.0 + jnp.exp(-gate)) * up).astype(jnp.bfloat16)

        def down_tile(cols):
            xr[p, :, cols] = dot(act, v_down[:, cols]).astype(jnp.bfloat16)

        col_loop(down_tile)
        for o in range(1, X_SIZE):
            r_copy(p, o).start()
        ret[p, lump(x), :] = xr[p, lump(x), :]
        streams(layer, 4, 6)
        for o in range(1, X_SIZE):
            r_copy(p, o).wait_recv()

        def comb_tile(cols):
            part[:, cols] = dot(comb[1], ret[p, :, cols])

        col_loop(comb_tile)

        for r in range(FAR_A):
            mine = part[rows_of(z - FAR_A + r), :]
            if r > 0:
                a_copy(p, r - 1).wait_recv()
                mine = mine + abuf[p, r].astype(jnp.float32)
            abuf[p, r] = mine.astype(jnp.bfloat16)
            a_copy(p, r).start()
            if r < FAR_B:
                mine = part[rows_of(z + FAR_B - r), :]
                if r > 0:
                    b_copy(p, r - 1).wait_recv()
                    mine = mine + bbuf[p, r].astype(jnp.float32)
                bbuf[p, r] = mine.astype(jnp.bfloat16)
                b_copy(p, r).start()
        b_copy(p, FAR_B - 1).wait_recv()
        a_copy(p, FAR_A - 1).wait_recv()
        total = (
            part[rows_of(z), :]
            + abuf[p, FAR_A].astype(jnp.float32)
            + bbuf[p, FAR_B].astype(jnp.float32)
        )
        obuf[p] = (obuf[1 - p].astype(jnp.float32) + total).astype(jnp.bfloat16)

        @pl.when(jnp.logical_not(o_is_self(layer)))
        def _():
            o_copy(p, layer).start()

        @pl.when(o_is_self(layer))
        def _():
            out[c, pl.ds(pl.multiple_of(quarter * own, own), own), :] = obuf[p]

    sends_done(1, layers - 1)

    @pl.loop(0, Y_SIZE)
    def _(q):
        @pl.loop(0, PIECES)
        def _(i):
            stream_done(q, i)

    for i in range(Y_SIZE):

        @pl.when(jnp.logical_and(quarter == y, quarter != i))
        def _():
            t_copy(i).wait_send()

    for m in range(micro):
        for zz in range(RING):

            @pl.when(jnp.logical_not(m_is_self(m, zz)))
            def _():
                m_copy(m, zz).wait_send()

    for m in range(micro):
        for i in range(Y_SIZE):

            @pl.when(jnp.logical_not(jnp.logical_and(quarter * CORES + m == sec, i == quarter)))
            def _():
                r = pl.ds(i * own, own)
                remote(
                    out.at[m, r],
                    out.at[m, r],
                    o_send.at[0],
                    o_recv.at[m, i],
                    (sec, right),
                ).wait_recv()


def per_device(tokens, norm_gain, w_gate, w_up, w_down, expert_ids, route_weight):
    micro, rows, width = tokens.shape
    layers = Y_SIZE * CORES
    own = rows // Y_SIZE
    every = RING * own
    lined = 2 * SLOT * X_SIZE
    hidden = w_gate.shape[-1]
    gains = lax.all_gather(norm_gain, "section", axis=0, tiled=True)
    dma = pltpu.SemaphoreType.DMA
    vmem = pl.BlockSpec(memory_space=pltpu.VMEM)
    hbm = pl.BlockSpec(memory_space=pl.ANY)
    bf16 = jnp.bfloat16
    result = pl.pallas_call(
        relay_kernel,
        out_shape=(
            jax.ShapeDtypeStruct((micro, rows, width), bf16),
            jax.ShapeDtypeStruct((layers, hidden, width), bf16),
            jax.ShapeDtypeStruct((layers, hidden, width), bf16),
            jax.ShapeDtypeStruct((layers, hidden, width), bf16),
        ),
        in_specs=[vmem, vmem, hbm, hbm, hbm, vmem, vmem],
        out_specs=(vmem, hbm, hbm, hbm),
        scratch_shapes=[
            pltpu.VMEM((hidden, width), bf16),
            pltpu.VMEM((hidden, width), bf16),
            pltpu.VMEM((hidden, width), bf16),
            pltpu.VMEM((micro, rows, LANES), bf16),
            pltpu.VMEM((layers, 2, rows, LANES), bf16),
            pltpu.VMEM((2, every, width), bf16),
            pltpu.VMEM((2, lined, width), bf16),
            pltpu.VMEM((2, lined, width), bf16),
            pltpu.VMEM((2, lined, width), bf16),
            pltpu.VMEM((2, every, lined), bf16),
            pltpu.VMEM((every, width), jnp.float32),
            pltpu.VMEM((2, FAR_A + 1, own, width), bf16),
            pltpu.VMEM((2, FAR_B + 1, own, width), bf16),
            pltpu.VMEM((2, own, width), bf16),
            dma((Y_SIZE, PIECES, 2, 3)),
            dma((Y_SIZE, PIECES, 2, 3)),
            dma((Y_SIZE, PIECES, 2, 3)),
            dma((Y_SIZE, PIECES, 2, 3)),
            dma((micro, RING)),
            dma((layers, 2)),
            dma((Y_SIZE,)),
            dma,
            dma((2, 2, FAR_A + 1)),
            dma((2, 2, FAR_A + 1)),
            dma((2, X_SIZE - 1)),
            dma((2, X_SIZE - 1)),
            dma((2, X_SIZE - 1)),
            dma((2, X_SIZE - 1)),
            dma((2, FAR_A)),
            dma((2, FAR_A)),
            dma((2, FAR_B)),
            dma((2, FAR_B)),
            dma((2,)),
            dma((micro, Y_SIZE)),
            dma((3,)),
        ],
        compiler_params=pltpu.CompilerParams(
            has_side_effects=True, vmem_limit_bytes=56_000_000
        ),
        name="relay",
    )(
        tokens,
        gains,
        w_gate[0, 0].T,
        w_up[0, 0].T,
        w_down[0, 0],
        expert_ids[0],
        route_weight[0],
    )
    return result[0][None]


def solution(mesh):
    return jax.shard_map(
        per_device,
        mesh=mesh,
        in_specs=(
            P(None, "expert", None),
            P("section", None),
            P("section", "expert", None, None),
            P("section", "expert", None, None),
            P("section", "expert", None, None),
            P("section", None, "expert", None),
            P("section", None, "expert", None),
        ),
        out_specs=P("section", None, "expert", None),
        check_vma=False,
    )
```

```python
import functools

import jax
import jax.numpy as jnp
from jax import lax
from jax.experimental import pallas as pl
from jax.experimental.pallas import tpu as pltpu
from jax.sharding import PartitionSpec as P

EPSILON = 1e-06
X_SIZE = 4
Y_SIZE = 4
CORES = 2
RING = 8
SLOT = 32
LANES = 128
COLS = 512
PIECES = 4
MESH = pl.DeviceIdType.MESH
LAG = 3
STRIPS = 2
START_GROUPS = PIECES + LAG
FAR_A = RING // 2
FAR_B = RING // 2 - 1


def relay_kernel(
    tokens,
    gains,
    w_gate,
    w_up,
    w_down,
    ids,
    route,
    out,
    f_gate,
    f_up,
    f_down,
    v_gate,
    v_up,
    v_down,
    local_meta,
    meta,
    ag,
    xs,
    xr,
    ret,
    comb,
    part,
    abuf,
    bbuf,
    obuf,
    y_send,
    y_recv,
    d_send,
    d_recv,
    m_send,
    m_recv,
    t_send,
    t_recv,
    z_send,
    z_recv,
    x_send,
    x_recv,
    r_send,
    r_recv,
    a_send,
    a_recv,
    b_send,
    b_recv,
    o_send,
    o_recv,
    v_sem,
):
    micro, rows, width = tokens.shape
    own = rows // Y_SIZE
    top = ids.shape[-1]
    experts = RING * X_SIZE
    layers = Y_SIZE * CORES
    lumps = 2 * SLOT
    every = RING * own
    tiles = width // COLS
    sec = lax.axis_index("section")
    pos = lax.axis_index("expert")
    y = sec // CORES
    c = sec % CORES
    z = pos // X_SIZE
    x = pos % X_SIZE
    half = z // Y_SIZE
    quarter = z % Y_SIZE

    def at(zz):
        return ((zz + 2 * RING) % RING) * X_SIZE + x

    right = at(z + 1)
    left = at(z - 1)
    sibling = y * CORES + 1 - c
    y_peer = (jnp.where(c == 0, y + 1, y + Y_SIZE - 1) % Y_SIZE) * CORES + c

    def remote(src, dst, send, recv, where):
        return pltpu.make_async_remote_copy(
            src_ref=src,
            dst_ref=dst,
            send_sem=send,
            recv_sem=recv,
            device_id=where,
            device_id_type=MESH,
        )

    def dot(a, b):
        return jnp.dot(a, b, preferred_element_type=jnp.float32)

    def dot_t(a, b):
        return lax.dot_general(
            a, b, (((1,), (1,)), ((), ())), preferred_element_type=jnp.float32
        )

    def col_loop(body, w):
        @pl.loop(w * (tiles // STRIPS), (w + 1) * (tiles // STRIPS))
        def _(i):
            body(pl.ds(pl.multiple_of(i * COLS, COLS), COLS))

    given = (w_gate, w_up, w_down)
    full = (f_gate, f_up, f_down)
    step = (
        w_gate.shape[0] // (2 * PIECES),
        w_up.shape[0] // (2 * PIECES),
        w_down.shape[0] // (2 * PIECES),
    )

    def part_rows(t, i, d):
        return pl.ds(pl.multiple_of((d * PIECES + i) * step[t], step[t]), step[t])

    def y_copy(src, l, i, t):
        r = part_rows(t, i, c)
        return remote(
            src.at[r], full[t].at[l, r], y_send.at[l, i, t], y_recv.at[l, i, t], (y_peer, pos)
        )

    def d_copy(src, l, i, d, t):
        r = part_rows(t, i, d)
        return remote(
            src.at[r],
            full[t].at[l, r],
            d_send.at[l, i, d, t],
            d_recv.at[l, i, d, t],
            (sibling, pos),
        )

    def away_from(l):
        q = l // CORES
        return jnp.where(c == 0, y - q + Y_SIZE, q - y + Y_SIZE) % Y_SIZE

    def stream(group, turn):
        for k in range(Y_SIZE):
            t = (turn - LAG * k) % 3
            g = group + (turn - LAG * k) // 3
            valid = jnp.logical_and(g >= 0, g < layers * PIECES)
            g = jnp.maximum(g, 0)
            l = g // PIECES
            i = g % PIECES
            here = jnp.logical_and(valid, away_from(l) == k)
            held = full[t].at[l]
            if k == 0:

                @pl.when(jnp.logical_and(here, l == sec))
                def _():
                    y_copy(given[t], l, i, t).start()
                    d_copy(given[t], l, i, 1 - c, t).start()
                    d_copy(given[t], l, i, c, t).start()

                @pl.when(jnp.logical_and(here, l != sec))
                def _():
                    d_copy(held, l, i, c, t).wait_recv()
                    y_copy(held, l, i, t).start()

            else:

                @pl.when(here)
                def _():
                    y_copy(held, l, i, t).wait_recv()
                    if k < Y_SIZE - 1:
                        y_copy(held, l, i, t).start()
                    d_copy(held, l, i, c, t).start()

    def stream_done(l, i):
        away = away_from(l)
        for t in range(3):
            held = full[t].at[l]

            @pl.when(away < Y_SIZE - 1)
            def _():
                y_copy(held, l, i, t).wait_send()

            @pl.when(jnp.logical_or(away > 0, l == sec))
            def _():
                d_copy(held, l, i, c, t).wait_send()

            @pl.when(l == sec)
            def _():
                d_copy(held, l, i, 1 - c, t).wait_send()

    def v_copy(src, dst, t):
        return pltpu.make_async_copy(src, dst, v_sem.at[t])

    held_v = (v_gate, v_up, v_down)

    def load_weights(layer):
        @pl.when(layer != sec)
        def _():
            for i in range(PIECES):
                for t in range(3):
                    d_copy(full[t].at[layer], layer, i, 1 - c, t).wait_recv()

        @pl.when(layer == sec)
        def _():
            for t in range(3):
                v_copy(given[t], held_v[t], t).start()

        @pl.when(layer != sec)
        def _():
            for t in range(3):
                v_copy(full[t].at[layer], held_v[t], t).start()

    def weights_ready(layer):
        for t in range(3):
            v_copy(full[t].at[layer], held_v[t], t).wait()

    lane = lax.broadcasted_iota(jnp.int32, (rows, LANES), 1)
    line = lax.broadcasted_iota(jnp.int32, (rows, LANES), 0)
    earlier = (lane < line).astype(jnp.bfloat16)

    def m_copy(m, zz):
        return remote(
            local_meta.at[m],
            meta.at[sec, half],
            m_send.at[m, zz],
            m_recv.at[sec, half],
            (quarter * CORES + m, at(zz)),
        )

    def m_is_self(m, zz):
        return jnp.logical_and(quarter * CORES + m == sec, zz == z)

    for m in range(micro):
        member = jnp.zeros((rows, LANES), jnp.float32)
        weight = jnp.zeros((rows, LANES), jnp.float32)
        for k in range(top):
            choice = ids[m, :, k : k + 1]
            member = member + (choice == lane).astype(jnp.float32)
            weight = weight + jnp.where(choice + experts == lane, route[m, :, k : k + 1], 0.0)
        before = dot(earlier, member.astype(jnp.bfloat16))
        slot = jnp.where(member > 0.0, before, -1.0)
        local_meta[m] = jnp.where(lane < experts, slot, weight).astype(jnp.bfloat16)

    def t_copy(i):
        return remote(
            tokens.at[c, pl.ds(i * own, own)],
            obuf.at[1],
            t_send.at[i],
            t_recv,
            (sec, at(half * Y_SIZE + i)),
        )

    for i in range(Y_SIZE):

        @pl.when(jnp.logical_and(quarter == y, quarter != i))
        def _():
            t_copy(i).start()

        @pl.when(jnp.logical_and(quarter == y, quarter == i))
        def _():
            obuf[1] = tokens[c, pl.ds(i * own, own), :]

    for m in range(micro):
        for zz in range(RING):

            @pl.when(jnp.logical_not(m_is_self(m, zz)))
            def _():
                m_copy(m, zz).start()

            @pl.when(m_is_self(m, zz))
            def _():
                meta[sec, half] = local_meta[m]

    @pl.loop(0, START_GROUPS)
    def _(g):
        for turn in range(3):
            stream(g, turn)

    @pl.when(quarter != y)
    def _():
        t_copy(0).wait_recv()

    wide = 4 * lumps
    w_lane = lax.broadcasted_iota(jnp.int32, (LANES, wide), 1)
    w_line = lax.broadcasted_iota(jnp.int32, (LANES, wide), 0)
    target = z * X_SIZE + w_lane // lumps
    spread_slot = (w_line == target).astype(jnp.bfloat16)
    spread_weight = (w_line == target + experts).astype(jnp.bfloat16)
    g_lane = lax.broadcasted_iota(jnp.int32, (rows, wide), 1)
    slot_of_lane = (g_lane % SLOT).astype(jnp.float32)
    block_of_lane = (g_lane // SLOT) % 2

    def rows_of(zz):
        return pl.ds(pl.multiple_of(((zz + 2 * RING) % RING) * own, own), own)

    def strip(w):
        return pl.ds(w * (width // STRIPS), width // STRIPS)

    def z_copy(p, k, d, src, w):
        return remote(
            ag.at[p, rows_of(src), strip(w)],
            ag.at[p, rows_of(src), strip(w)],
            z_send.at[p, d, k, w],
            z_recv.at[p, d, k, w],
            (sec, (right, left)[d]),
        )

    def lump(d):
        return pl.ds(pl.multiple_of(d * lumps, lumps), lumps)

    def x_copy(p, o, w):
        return remote(
            xs.at[p, lump((x + o) % X_SIZE), strip(w)],
            xr.at[p, lump(x), strip(w)],
            x_send.at[p, o - 1, w],
            x_recv.at[p, o - 1, w],
            (sec, z * X_SIZE + (x + o) % X_SIZE),
        )

    def r_copy(p, o, w):
        return remote(
            xr.at[p, lump((x + o) % X_SIZE), strip(w)],
            ret.at[p, lump(x), strip(w)],
            r_send.at[p, o - 1, w],
            r_recv.at[p, o - 1, w],
            (sec, z * X_SIZE + (x + o) % X_SIZE),
        )

    def a_copy(p, r, w):
        return remote(
            abuf.at[p, r, :, strip(w)],
            abuf.at[p, r + 1, :, strip(w)],
            a_send.at[p, r, w],
            a_recv.at[p, r, w],
            (sec, left),
        )

    def b_copy(p, r, w):
        return remote(
            bbuf.at[p, r, :, strip(w)],
            bbuf.at[p, r + 1, :, strip(w)],
            b_send.at[p, r, w],
            b_recv.at[p, r, w],
            (sec, right),
        )

    home = half * Y_SIZE + y

    def o_copy(p, layer):
        return remote(
            obuf.at[p],
            out.at[c, pl.ds(pl.multiple_of(quarter * own, own), own)],
            o_send.at[p],
            o_recv.at[c, quarter],
            (layer, at(home)),
        )

    def o_is_self(layer):
        return jnp.logical_and(layer == sec, home == z)

    def sends_done(p, layer):
        for w in range(STRIPS):
            for k in range(1, FAR_A + 1):
                z_copy(p, k, 0, z, w).wait_send()
            for k in range(1, FAR_B + 1):
                z_copy(p, k, 1, z, w).wait_send()
            for o in range(1, X_SIZE):
                x_copy(p, o, w).wait_send()
                r_copy(p, o, w).wait_send()
            for r in range(FAR_A):
                a_copy(p, r, w).wait_send()
            for r in range(FAR_B):
                b_copy(p, r, w).wait_send()

        @pl.when(jnp.logical_not(o_is_self(layer)))
        def _():
            o_copy(p, layer).wait_send()

    def groups_at(layer, at_point):
        count = START_GROUPS + PIECES * layer + at_point
        return jnp.minimum(count, layers * PIECES + LAG)

    def streams(layer, at_point):
        @pl.loop(groups_at(layer, at_point), groups_at(layer, at_point + 1))
        def _(g):
            for turn in range(3):
                stream(g, turn)

    @pl.loop(0, layers)
    def _(layer):
        p = layer % 2

        value = obuf[1 - p].astype(jnp.float32)
        inverse = lax.rsqrt(jnp.mean(value * value, axis=-1, keepdims=True) + EPSILON)
        gain = gains[pl.ds(layer, 1), :]
        ag[p, rows_of(z), :] = (value * inverse * gain).astype(jnp.bfloat16)
        for w in range(STRIPS):
            z_copy(p, 1, 0, z, w).start()
            z_copy(p, 1, 1, z, w).start()
        load_weights(layer)
        streams(layer, 0)
        for h in range(2):

            @pl.when(jnp.logical_not(jnp.logical_and(layer == sec, home - half * Y_SIZE + h * Y_SIZE == z)))
            def _():
                remote(
                    meta.at[layer, h],
                    meta.at[layer, h],
                    m_send.at[0, 0],
                    m_recv.at[layer, h],
                    (sec, right),
                ).wait_recv()

        for k in range(1, FAR_A):
            for w in range(STRIPS):
                z_copy(p, k, 0, z - k, w).wait_recv()
                z_copy(p, k + 1, 0, z - k, w).start()
                z_copy(p, k, 1, z + k, w).wait_recv()
                if k < FAR_B:
                    z_copy(p, k + 1, 1, z + k, w).start()
            if k == 2:
                streams(layer, 1)

        @pl.when(layer >= 1)
        def _():
            sends_done(1 - p, layer - 1)

        for h in range(2):
            table = meta[layer, h]
            hit = jnp.logical_and(dot(table, spread_slot) == slot_of_lane, block_of_lane == h)
            scaled = jnp.where(hit, dot(table, spread_weight), 0.0)
            comb[0, pl.ds(h * rows, rows), :] = hit.astype(jnp.float32).astype(jnp.bfloat16)
            comb[1, pl.ds(h * rows, rows), :] = scaled.astype(jnp.bfloat16)
        pick = jnp.transpose(comb[0].astype(jnp.float32)).astype(jnp.bfloat16)

        for w in range(STRIPS):
            z_copy(p, FAR_A, 0, z - FAR_A, w).wait_recv()

            def pick_tile(cols):
                xs[p, :, cols] = dot(pick, ag[p, :, cols]).astype(jnp.bfloat16)

            col_loop(pick_tile, w)
            for o in range(1, X_SIZE):
                x_copy(p, o, w).start()
            xr[p, lump(x), strip(w)] = xs[p, lump(x), strip(w)]
        streams(layer, 2)
        weights_ready(layer)
        gate = 0.0
        up = 0.0
        for w in range(STRIPS):
            for o in range(1, X_SIZE):
                x_copy(p, o, w).wait_recv()
            gate = gate + dot_t(xr[p, :, strip(w)], v_gate[:, strip(w)])
            up = up + dot_t(xr[p, :, strip(w)], v_up[:, strip(w)])
        act = (gate / (1.0 + jnp.exp(-gate)) * up).astype(jnp.bfloat16)
        for w in range(STRIPS):

            def down_tile(cols):
                xr[p, :, cols] = dot(act, v_down[:, cols]).astype(jnp.bfloat16)

            col_loop(down_tile, w)
            for o in range(1, X_SIZE):
                r_copy(p, o, w).start()
            ret[p, lump(x), strip(w)] = xr[p, lump(x), strip(w)]
        streams(layer, 3)

        for r in range(FAR_A):
            for w in range(STRIPS):
                if r == 0:
                    for o in range(1, X_SIZE):
                        r_copy(p, o, w).wait_recv()

                    def comb_tile(cols):
                        part[:, cols] = dot(comb[1], ret[p, :, cols])

                    col_loop(comb_tile, w)
                mine = part[rows_of(z - FAR_A + r), strip(w)]
                if r > 0:
                    a_copy(p, r - 1, w).wait_recv()
                    mine = mine + abuf[p, r, :, strip(w)].astype(jnp.float32)
                abuf[p, r, :, strip(w)] = mine.astype(jnp.bfloat16)
                a_copy(p, r, w).start()
                if r < FAR_B:
                    mine = part[rows_of(z + FAR_B - r), strip(w)]
                    if r > 0:
                        b_copy(p, r - 1, w).wait_recv()
                        mine = mine + bbuf[p, r, :, strip(w)].astype(jnp.float32)
                    bbuf[p, r, :, strip(w)] = mine.astype(jnp.bfloat16)
                    b_copy(p, r, w).start()
        for w in range(STRIPS):
            b_copy(p, FAR_B - 1, w).wait_recv()
            a_copy(p, FAR_A - 1, w).wait_recv()
            total = (
                part[rows_of(z), strip(w)]
                + abuf[p, FAR_A, :, strip(w)].astype(jnp.float32)
                + bbuf[p, FAR_B, :, strip(w)].astype(jnp.float32)
            )
            obuf[p, :, strip(w)] = (
                obuf[1 - p, :, strip(w)].astype(jnp.float32) + total
            ).astype(jnp.bfloat16)

        @pl.when(jnp.logical_not(o_is_self(layer)))
        def _():
            o_copy(p, layer).start()

        @pl.when(o_is_self(layer))
        def _():
            out[c, pl.ds(pl.multiple_of(quarter * own, own), own), :] = obuf[p]

    sends_done(1, layers - 1)

    @pl.loop(0, layers)
    def _(l):
        @pl.loop(0, PIECES)
        def _(i):
            stream_done(l, i)

    for i in range(Y_SIZE):

        @pl.when(jnp.logical_and(quarter == y, quarter != i))
        def _():
            t_copy(i).wait_send()

    for m in range(micro):
        for zz in range(RING):

            @pl.when(jnp.logical_not(m_is_self(m, zz)))
            def _():
                m_copy(m, zz).wait_send()

    for m in range(micro):
        for i in range(Y_SIZE):

            @pl.when(jnp.logical_not(jnp.logical_and(quarter * CORES + m == sec, i == quarter)))
            def _():
                r = pl.ds(i * own, own)
                remote(
                    out.at[m, r],
                    out.at[m, r],
                    o_send.at[0],
                    o_recv.at[m, i],
                    (sec, right),
                ).wait_recv()


def per_device(tokens, norm_gain, w_gate, w_up, w_down, expert_ids, route_weight):
    micro, rows, width = tokens.shape
    layers = Y_SIZE * CORES
    own = rows // Y_SIZE
    every = RING * own
    lined = 2 * SLOT * X_SIZE
    hidden = w_gate.shape[-1]
    gains = lax.all_gather(norm_gain, "section", axis=0, tiled=True)
    dma = pltpu.SemaphoreType.DMA
    vmem = pl.BlockSpec(memory_space=pltpu.VMEM)
    hbm = pl.BlockSpec(memory_space=pl.ANY)
    bf16 = jnp.bfloat16
    result = pl.pallas_call(
        relay_kernel,
        out_shape=(
            jax.ShapeDtypeStruct((micro, rows, width), bf16),
            jax.ShapeDtypeStruct((layers, hidden, width), bf16),
            jax.ShapeDtypeStruct((layers, hidden, width), bf16),
            jax.ShapeDtypeStruct((layers, hidden, width), bf16),
        ),
        in_specs=[vmem, vmem, hbm, hbm, hbm, vmem, vmem],
        out_specs=(vmem, hbm, hbm, hbm),
        scratch_shapes=[
            pltpu.VMEM((hidden, width), bf16),
            pltpu.VMEM((hidden, width), bf16),
            pltpu.VMEM((hidden, width), bf16),
            pltpu.VMEM((micro, rows, LANES), bf16),
            pltpu.VMEM((layers, 2, rows, LANES), bf16),
            pltpu.VMEM((2, every, width), bf16),
            pltpu.VMEM((2, lined, width), bf16),
            pltpu.VMEM((2, lined, width), bf16),
            pltpu.VMEM((2, lined, width), bf16),
            pltpu.VMEM((2, every, lined), bf16),
            pltpu.VMEM((every, width), jnp.float32),
            pltpu.VMEM((2, FAR_A + 1, own, width), bf16),
            pltpu.VMEM((2, FAR_B + 1, own, width), bf16),
            pltpu.VMEM((2, own, width), bf16),
            dma((layers, PIECES, 3)),
            dma((layers, PIECES, 3)),
            dma((layers, PIECES, 2, 3)),
            dma((layers, PIECES, 2, 3)),
            dma((micro, RING)),
            dma((layers, 2)),
            dma((Y_SIZE,)),
            dma,
            dma((2, 2, FAR_A + 1, STRIPS)),
            dma((2, 2, FAR_A + 1, STRIPS)),
            dma((2, X_SIZE - 1, STRIPS)),
            dma((2, X_SIZE - 1, STRIPS)),
            dma((2, X_SIZE - 1, STRIPS)),
            dma((2, X_SIZE - 1, STRIPS)),
            dma((2, FAR_A, STRIPS)),
            dma((2, FAR_A, STRIPS)),
            dma((2, FAR_B, STRIPS)),
            dma((2, FAR_B, STRIPS)),
            dma((2,)),
            dma((micro, Y_SIZE)),
            dma((3,)),
        ],
        compiler_params=pltpu.CompilerParams(
            has_side_effects=True, vmem_limit_bytes=56_000_000
        ),
        name="relay",
    )(
        tokens,
        gains,
        w_gate[0, 0].T,
        w_up[0, 0].T,
        w_down[0, 0],
        expert_ids[0],
        route_weight[0],
    )
    return result[0][None]


def solution(mesh):
    return jax.shard_map(
        per_device,
        mesh=mesh,
        in_specs=(
            P(None, "expert", None),
            P("section", None),
            P("section", "expert", None, None),
            P("section", "expert", None, None),
            P("section", "expert", None, None),
            P("section", None, "expert", None),
            P("section", None, "expert", None),
        ),
        out_specs=P("section", None, "expert", None),
        check_vma=False,
    )
```

```python
import functools

import jax
import jax.numpy as jnp
from jax import lax
from jax.experimental import pallas as pl
from jax.experimental.pallas import tpu as pltpu
from jax.sharding import PartitionSpec as P

EPSILON = 1e-06
X_SIZE = 4
Y_SIZE = 4
CORES = 2
RING = 8
SLOT = 32
LANES = 128
COLS = 512
PIECES = 4
MESH = pl.DeviceIdType.MESH
LAG = 3
STRIPS = 4
START_GROUPS = PIECES + LAG
FAR_A = RING // 2
FAR_B = RING // 2 - 1


def relay_kernel(
    tokens,
    own_gain,
    w_gate,
    w_up,
    w_down,
    ids,
    route,
    out,
    f_gate,
    f_up,
    f_down,
    v_gate,
    v_up,
    v_down,
    local_meta,
    meta,
    ag,
    xs,
    xr,
    ret,
    comb,
    part,
    abuf,
    bbuf,
    obuf,
    gains,
    g_send,
    g_recv,
    y_send,
    y_recv,
    d_send,
    d_recv,
    m_send,
    m_recv,
    t_send,
    t_recv,
    z_send,
    z_recv,
    x_send,
    x_recv,
    r_send,
    r_recv,
    a_send,
    a_recv,
    b_send,
    b_recv,
    o_send,
    o_recv,
    v_sem,
):
    micro, rows, width = tokens.shape
    own = rows // Y_SIZE
    top = ids.shape[-1]
    experts = RING * X_SIZE
    layers = Y_SIZE * CORES
    lumps = 2 * SLOT
    every = RING * own
    tiles = width // COLS
    sec = lax.axis_index("section")
    pos = lax.axis_index("expert")
    y = sec // CORES
    c = sec % CORES
    z = pos // X_SIZE
    x = pos % X_SIZE
    half = z // Y_SIZE
    quarter = z % Y_SIZE

    def at(zz):
        return ((zz + 2 * RING) % RING) * X_SIZE + x

    right = at(z + 1)
    left = at(z - 1)
    sibling = y * CORES + 1 - c
    y_peer = (jnp.where(c == 0, y + 1, y + Y_SIZE - 1) % Y_SIZE) * CORES + c

    def remote(src, dst, send, recv, where):
        return pltpu.make_async_remote_copy(
            src_ref=src,
            dst_ref=dst,
            send_sem=send,
            recv_sem=recv,
            device_id=where,
            device_id_type=MESH,
        )

    def dot(a, b):
        return jnp.dot(a, b, preferred_element_type=jnp.float32)

    def dot_t(a, b):
        return lax.dot_general(
            a, b, (((1,), (1,)), ((), ())), preferred_element_type=jnp.float32
        )

    def col_loop(body, w):
        @pl.loop(w * (tiles // STRIPS), (w + 1) * (tiles // STRIPS))
        def _(i):
            body(pl.ds(pl.multiple_of(i * COLS, COLS), COLS))

    given = (w_gate, w_up, w_down)
    full = (f_gate, f_up, f_down)
    step = (
        w_gate.shape[0] // (2 * PIECES),
        w_up.shape[0] // (2 * PIECES),
        w_down.shape[0] // (2 * PIECES),
    )

    def part_rows(t, i, d):
        return pl.ds(pl.multiple_of((d * PIECES + i) * step[t], step[t]), step[t])

    def y_copy(src, l, i, t):
        r = part_rows(t, i, c)
        return remote(
            src.at[r], full[t].at[l, r], y_send.at[l, i, t], y_recv.at[l, i, t], (y_peer, pos)
        )

    def d_copy(src, l, i, d, t):
        r = part_rows(t, i, d)
        return remote(
            src.at[r],
            full[t].at[l, r],
            d_send.at[l, i, d, t],
            d_recv.at[l, i, d, t],
            (sibling, pos),
        )

    def away_from(l):
        q = l // CORES
        return jnp.where(c == 0, y - q + Y_SIZE, q - y + Y_SIZE) % Y_SIZE

    def stream(group, turn):
        for k in range(Y_SIZE):
            t = (turn - LAG * k) % 3
            g = group + (turn - LAG * k) // 3
            valid = jnp.logical_and(g >= 0, g < layers * PIECES)
            g = jnp.maximum(g, 0)
            l = g // PIECES
            i = g % PIECES
            here = jnp.logical_and(valid, away_from(l) == k)
            held = full[t].at[l]
            if k == 0:

                @pl.when(jnp.logical_and(here, l == sec))
                def _():
                    y_copy(given[t], l, i, t).start()
                    d_copy(given[t], l, i, 1 - c, t).start()
                    d_copy(given[t], l, i, c, t).start()

                @pl.when(jnp.logical_and(here, l != sec))
                def _():
                    d_copy(held, l, i, c, t).wait_recv()
                    y_copy(held, l, i, t).start()

            else:

                @pl.when(here)
                def _():
                    y_copy(held, l, i, t).wait_recv()
                    if k < Y_SIZE - 1:
                        y_copy(held, l, i, t).start()
                    d_copy(held, l, i, c, t).start()

    def stream_done(l, i):
        away = away_from(l)
        for t in range(3):
            held = full[t].at[l]

            @pl.when(away < Y_SIZE - 1)
            def _():
                y_copy(held, l, i, t).wait_send()

            @pl.when(jnp.logical_or(away > 0, l == sec))
            def _():
                d_copy(held, l, i, c, t).wait_send()

            @pl.when(l == sec)
            def _():
                d_copy(held, l, i, 1 - c, t).wait_send()

    def v_copy(src, dst, t):
        return pltpu.make_async_copy(src, dst, v_sem.at[t])

    held_v = (v_gate, v_up, v_down)

    def load_weights(layer):
        @pl.when(layer != sec)
        def _():
            for i in range(PIECES):
                for t in range(3):
                    d_copy(full[t].at[layer], layer, i, 1 - c, t).wait_recv()

        @pl.when(layer == sec)
        def _():
            for t in range(3):
                v_copy(given[t], held_v[t], t).start()

        @pl.when(layer != sec)
        def _():
            for t in range(3):
                v_copy(full[t].at[layer], held_v[t], t).start()

    def weights_ready(layer):
        for t in range(3):
            v_copy(full[t].at[layer], held_v[t], t).wait()

    lane = lax.broadcasted_iota(jnp.int32, (rows, LANES), 1)
    line = lax.broadcasted_iota(jnp.int32, (rows, LANES), 0)
    earlier = (lane < line).astype(jnp.bfloat16)

    def m_copy(m, zz):
        return remote(
            local_meta.at[m],
            meta.at[sec, half],
            m_send.at[m, zz],
            m_recv.at[sec, half],
            (quarter * CORES + m, at(zz)),
        )

    def m_is_self(m, zz):
        return jnp.logical_and(quarter * CORES + m == sec, zz == z)

    for m in range(micro):
        member = jnp.zeros((rows, LANES), jnp.float32)
        weight = jnp.zeros((rows, LANES), jnp.float32)
        for k in range(top):
            choice = ids[m, :, k : k + 1]
            member = member + (choice == lane).astype(jnp.float32)
            weight = weight + jnp.where(choice + experts == lane, route[m, :, k : k + 1], 0.0)
        before = dot(earlier, member.astype(jnp.bfloat16))
        slot = jnp.where(member > 0.0, before, -1.0)
        local_meta[m] = jnp.where(lane < experts, slot, weight).astype(jnp.bfloat16)

    def g_copy(other):
        return remote(
            own_gain, gains.at[sec], g_send.at[other], g_recv.at[sec], (other, pos)
        )

    gains[sec] = own_gain[...]

    def t_copy(i):
        return remote(
            tokens.at[c, pl.ds(i * own, own)],
            obuf.at[1],
            t_send.at[i],
            t_recv,
            (sec, at(half * Y_SIZE + i)),
        )

    for i in range(Y_SIZE):

        @pl.when(jnp.logical_and(quarter == y, quarter != i))
        def _():
            t_copy(i).start()

        @pl.when(jnp.logical_and(quarter == y, quarter == i))
        def _():
            obuf[1] = tokens[c, pl.ds(i * own, own), :]

    for m in range(micro):
        for zz in range(RING):

            @pl.when(jnp.logical_not(m_is_self(m, zz)))
            def _():
                m_copy(m, zz).start()

            @pl.when(m_is_self(m, zz))
            def _():
                meta[sec, half] = local_meta[m]

    for other in range(layers):

        @pl.when(sec != other)
        def _():
            g_copy(other).start()

    @pl.loop(0, START_GROUPS)
    def _(g):
        for turn in range(3):
            stream(g, turn)

    @pl.when(quarter != y)
    def _():
        t_copy(0).wait_recv()

    wide = 4 * lumps
    w_lane = lax.broadcasted_iota(jnp.int32, (LANES, wide), 1)
    w_line = lax.broadcasted_iota(jnp.int32, (LANES, wide), 0)
    target = z * X_SIZE + w_lane // lumps
    spread_slot = (w_line == target).astype(jnp.bfloat16)
    spread_weight = (w_line == target + experts).astype(jnp.bfloat16)
    g_lane = lax.broadcasted_iota(jnp.int32, (rows, wide), 1)
    slot_of_lane = (g_lane % SLOT).astype(jnp.float32)
    block_of_lane = (g_lane // SLOT) % 2

    def rows_of(zz):
        return pl.ds(pl.multiple_of(((zz + 2 * RING) % RING) * own, own), own)

    def strip(w):
        return pl.ds(w * (width // STRIPS), width // STRIPS)

    def z_copy(p, k, d, src, w):
        return remote(
            ag.at[p, rows_of(src), strip(w)],
            ag.at[p, rows_of(src), strip(w)],
            z_send.at[p, d, k, w],
            z_recv.at[p, d, k, w],
            (sec, (right, left)[d]),
        )

    def lump(d):
        return pl.ds(pl.multiple_of(d * lumps, lumps), lumps)

    def x_copy(p, o, w):
        return remote(
            xs.at[p, lump((x + o) % X_SIZE), strip(w)],
            xr.at[p, lump(x), strip(w)],
            x_send.at[p, o - 1, w],
            x_recv.at[p, o - 1, w],
            (sec, z * X_SIZE + (x + o) % X_SIZE),
        )

    def r_copy(p, o, w):
        return remote(
            xr.at[p, lump((x + o) % X_SIZE), strip(w)],
            ret.at[p, lump(x), strip(w)],
            r_send.at[p, o - 1, w],
            r_recv.at[p, o - 1, w],
            (sec, z * X_SIZE + (x + o) % X_SIZE),
        )

    def a_copy(p, r, w):
        return remote(
            abuf.at[p, r, :, strip(w)],
            abuf.at[p, r + 1, :, strip(w)],
            a_send.at[p, r, w],
            a_recv.at[p, r, w],
            (sec, left),
        )

    def b_copy(p, r, w):
        return remote(
            bbuf.at[p, r, :, strip(w)],
            bbuf.at[p, r + 1, :, strip(w)],
            b_send.at[p, r, w],
            b_recv.at[p, r, w],
            (sec, right),
        )

    home = half * Y_SIZE + y

    def o_copy(p, layer):
        return remote(
            obuf.at[p],
            out.at[c, pl.ds(pl.multiple_of(quarter * own, own), own)],
            o_send.at[p],
            o_recv.at[c, quarter],
            (layer, at(home)),
        )

    def o_is_self(layer):
        return jnp.logical_and(layer == sec, home == z)

    def sends_done(p, layer):
        for w in range(STRIPS):
            for k in range(1, FAR_A + 1):
                z_copy(p, k, 0, z, w).wait_send()
            for k in range(1, FAR_B + 1):
                z_copy(p, k, 1, z, w).wait_send()
            for o in range(1, X_SIZE):
                x_copy(p, o, w).wait_send()
                r_copy(p, o, w).wait_send()
            for r in range(FAR_A):
                a_copy(p, r, w).wait_send()
            for r in range(FAR_B):
                b_copy(p, r, w).wait_send()

        @pl.when(jnp.logical_not(o_is_self(layer)))
        def _():
            o_copy(p, layer).wait_send()

    def groups_at(layer, at_point):
        count = START_GROUPS + PIECES * layer + at_point
        return jnp.minimum(count, layers * PIECES + LAG)

    def streams(layer, at_point):
        @pl.loop(groups_at(layer, at_point), groups_at(layer, at_point + 1))
        def _(g):
            for turn in range(3):
                stream(g, turn)

    @pl.loop(0, layers)
    def _(layer):
        p = layer % 2

        value = obuf[1 - p].astype(jnp.float32)
        inverse = lax.rsqrt(jnp.mean(value * value, axis=-1, keepdims=True) + EPSILON)

        @pl.when(layer != sec)
        def _():
            remote(
                gains.at[layer], gains.at[layer], g_send.at[0], g_recv.at[layer], (sec, right)
            ).wait_recv()

        gain = gains[layer]
        ag[p, rows_of(z), :] = (value * inverse * gain).astype(jnp.bfloat16)
        for w in range(STRIPS):
            z_copy(p, 1, 0, z, w).start()
            z_copy(p, 1, 1, z, w).start()
        load_weights(layer)
        streams(layer, 0)
        for h in range(2):

            @pl.when(jnp.logical_not(jnp.logical_and(layer == sec, home - half * Y_SIZE + h * Y_SIZE == z)))
            def _():
                remote(
                    meta.at[layer, h],
                    meta.at[layer, h],
                    m_send.at[0, 0],
                    m_recv.at[layer, h],
                    (sec, right),
                ).wait_recv()

        for k in range(1, FAR_A):
            for w in range(STRIPS):
                z_copy(p, k, 0, z - k, w).wait_recv()
                z_copy(p, k + 1, 0, z - k, w).start()
                z_copy(p, k, 1, z + k, w).wait_recv()
                if k < FAR_B:
                    z_copy(p, k + 1, 1, z + k, w).start()
            if k == 2:
                streams(layer, 1)

        @pl.when(layer >= 1)
        def _():
            sends_done(1 - p, layer - 1)

        for h in range(2):
            table = meta[layer, h]
            hit = jnp.logical_and(dot(table, spread_slot) == slot_of_lane, block_of_lane == h)
            scaled = jnp.where(hit, dot(table, spread_weight), 0.0)
            comb[0, pl.ds(h * rows, rows), :] = hit.astype(jnp.float32).astype(jnp.bfloat16)
            comb[1, pl.ds(h * rows, rows), :] = scaled.astype(jnp.bfloat16)
        pick = jnp.transpose(comb[0].astype(jnp.float32)).astype(jnp.bfloat16)

        for w in range(STRIPS):
            z_copy(p, FAR_A, 0, z - FAR_A, w).wait_recv()

            def pick_tile(cols):
                xs[p, :, cols] = dot(pick, ag[p, :, cols]).astype(jnp.bfloat16)

            col_loop(pick_tile, w)
            for o in range(1, X_SIZE):
                x_copy(p, o, w).start()
            xr[p, lump(x), strip(w)] = xs[p, lump(x), strip(w)]
        streams(layer, 2)
        weights_ready(layer)
        gate = 0.0
        up = 0.0
        for w in range(STRIPS):
            for o in range(1, X_SIZE):
                x_copy(p, o, w).wait_recv()
            gate = gate + dot_t(xr[p, :, strip(w)], v_gate[:, strip(w)])
            up = up + dot_t(xr[p, :, strip(w)], v_up[:, strip(w)])
        act = (gate / (1.0 + jnp.exp(-gate)) * up).astype(jnp.bfloat16)
        for w in range(STRIPS):

            def down_tile(cols):
                xr[p, :, cols] = dot(act, v_down[:, cols]).astype(jnp.bfloat16)

            col_loop(down_tile, w)
            for o in range(1, X_SIZE):
                r_copy(p, o, w).start()
            ret[p, lump(x), strip(w)] = xr[p, lump(x), strip(w)]
        streams(layer, 3)

        for r in range(FAR_A):
            for w in range(STRIPS):
                if r == 0:
                    for o in range(1, X_SIZE):
                        r_copy(p, o, w).wait_recv()

                    def comb_tile(cols):
                        part[:, cols] = dot(comb[1], ret[p, :, cols])

                    col_loop(comb_tile, w)
                mine = part[rows_of(z - FAR_A + r), strip(w)]
                if r > 0:
                    a_copy(p, r - 1, w).wait_recv()
                    mine = mine + abuf[p, r, :, strip(w)].astype(jnp.float32)
                abuf[p, r, :, strip(w)] = mine.astype(jnp.bfloat16)
                a_copy(p, r, w).start()
                if r < FAR_B:
                    mine = part[rows_of(z + FAR_B - r), strip(w)]
                    if r > 0:
                        b_copy(p, r - 1, w).wait_recv()
                        mine = mine + bbuf[p, r, :, strip(w)].astype(jnp.float32)
                    bbuf[p, r, :, strip(w)] = mine.astype(jnp.bfloat16)
                    b_copy(p, r, w).start()
        for w in range(STRIPS):
            b_copy(p, FAR_B - 1, w).wait_recv()
            a_copy(p, FAR_A - 1, w).wait_recv()
            total = (
                part[rows_of(z), strip(w)]
                + abuf[p, FAR_A, :, strip(w)].astype(jnp.float32)
                + bbuf[p, FAR_B, :, strip(w)].astype(jnp.float32)
            )
            obuf[p, :, strip(w)] = (
                obuf[1 - p, :, strip(w)].astype(jnp.float32) + total
            ).astype(jnp.bfloat16)

        @pl.when(jnp.logical_not(o_is_self(layer)))
        def _():
            o_copy(p, layer).start()

        @pl.when(o_is_self(layer))
        def _():
            out[c, pl.ds(pl.multiple_of(quarter * own, own), own), :] = obuf[p]

    for other in range(layers):

        @pl.when(sec != other)
        def _():
            g_copy(other).wait_send()

    sends_done(1, layers - 1)

    @pl.loop(0, layers)
    def _(l):
        @pl.loop(0, PIECES)
        def _(i):
            stream_done(l, i)

    for i in range(Y_SIZE):

        @pl.when(jnp.logical_and(quarter == y, quarter != i))
        def _():
            t_copy(i).wait_send()

    for m in range(micro):
        for zz in range(RING):

            @pl.when(jnp.logical_not(m_is_self(m, zz)))
            def _():
                m_copy(m, zz).wait_send()

    for m in range(micro):
        for i in range(Y_SIZE):

            @pl.when(jnp.logical_not(jnp.logical_and(quarter * CORES + m == sec, i == quarter)))
            def _():
                r = pl.ds(i * own, own)
                remote(
                    out.at[m, r],
                    out.at[m, r],
                    o_send.at[0],
                    o_recv.at[m, i],
                    (sec, right),
                ).wait_recv()


def per_device(tokens, norm_gain, w_gate, w_up, w_down, expert_ids, route_weight):
    micro, rows, width = tokens.shape
    layers = Y_SIZE * CORES
    own = rows // Y_SIZE
    every = RING * own
    lined = 2 * SLOT * X_SIZE
    hidden = w_gate.shape[-1]
    dma = pltpu.SemaphoreType.DMA
    vmem = pl.BlockSpec(memory_space=pltpu.VMEM)
    hbm = pl.BlockSpec(memory_space=pl.ANY)
    bf16 = jnp.bfloat16
    result = pl.pallas_call(
        relay_kernel,
        out_shape=(
            jax.ShapeDtypeStruct((micro, rows, width), bf16),
            jax.ShapeDtypeStruct((layers, hidden, width), bf16),
            jax.ShapeDtypeStruct((layers, hidden, width), bf16),
            jax.ShapeDtypeStruct((layers, hidden, width), bf16),
        ),
        in_specs=[vmem, vmem, hbm, hbm, hbm, vmem, vmem],
        out_specs=(vmem, hbm, hbm, hbm),
        scratch_shapes=[
            pltpu.VMEM((hidden, width), bf16),
            pltpu.VMEM((hidden, width), bf16),
            pltpu.VMEM((hidden, width), bf16),
            pltpu.VMEM((micro, rows, LANES), bf16),
            pltpu.VMEM((layers, 2, rows, LANES), bf16),
            pltpu.VMEM((2, every, width), bf16),
            pltpu.VMEM((2, lined, width), bf16),
            pltpu.VMEM((2, lined, width), bf16),
            pltpu.VMEM((2, lined, width), bf16),
            pltpu.VMEM((2, every, lined), bf16),
            pltpu.VMEM((every, width), jnp.float32),
            pltpu.VMEM((2, FAR_A + 1, own, width), bf16),
            pltpu.VMEM((2, FAR_B + 1, own, width), bf16),
            pltpu.VMEM((2, own, width), bf16),
            pltpu.VMEM((layers, 1, width), jnp.float32),
            dma((layers,)),
            dma((layers,)),
            dma((layers, PIECES, 3)),
            dma((layers, PIECES, 3)),
            dma((layers, PIECES, 2, 3)),
            dma((layers, PIECES, 2, 3)),
            dma((micro, RING)),
            dma((layers, 2)),
            dma((Y_SIZE,)),
            dma,
            dma((2, 2, FAR_A + 1, STRIPS)),
            dma((2, 2, FAR_A + 1, STRIPS)),
            dma((2, X_SIZE - 1, STRIPS)),
            dma((2, X_SIZE - 1, STRIPS)),
            dma((2, X_SIZE - 1, STRIPS)),
            dma((2, X_SIZE - 1, STRIPS)),
            dma((2, FAR_A, STRIPS)),
            dma((2, FAR_A, STRIPS)),
            dma((2, FAR_B, STRIPS)),
            dma((2, FAR_B, STRIPS)),
            dma((2,)),
            dma((micro, Y_SIZE)),
            dma((3,)),
        ],
        compiler_params=pltpu.CompilerParams(
            has_side_effects=True, vmem_limit_bytes=56_000_000
        ),
        name="relay",
    )(
        tokens,
        norm_gain,
        w_gate[0, 0].T,
        w_up[0, 0].T,
        w_down[0, 0],
        expert_ids[0],
        route_weight[0],
    )
    return result[0][None]


def solution(mesh):
    return jax.shard_map(
        per_device,
        mesh=mesh,
        in_specs=(
            P(None, "expert", None),
            P("section", None),
            P("section", "expert", None, None),
            P("section", "expert", None, None),
            P("section", "expert", None, None),
            P("section", None, "expert", None),
            P("section", None, "expert", None),
        ),
        out_specs=P("section", None, "expert", None),
        check_vma=False,
    )
```
